128 devices in a mesh: dp: 8 (over z, y_lo), tensor: 16 (over x, y_hi, core).
Axes of the slice: x: 4, y: 4 (y_hi: 2, y_lo: 2; y = y_hi * 2 + y_lo), z: 4, core: 2. Of those that a mesh axis runs over, the one named last changes fastest.
Arguments:
- tokens: bfloat16 [2048, 4096], P(('dp', 'tensor')), may hold values from -4 to 4
- lengths: int32 [8], replicated, may hold values from 64 to 256, as said below
- norm_gains: float32 [2, 4096], replicated, may hold values from 0.25 to 1.75
- query_weight: bfloat16 [2, 4096, 4096], P(None, None, 'tensor'), may hold values from -0.09375 to 0.09375
- key_weight: bfloat16 [2, 4096, 1024], P(None, None, 'tensor'), may hold values from -0.09375 to 0.09375
- value_weight: bfloat16 [2, 4096, 1024], P(None, None, 'tensor'), may hold values from -0.09375 to 0.09375
- out_weight: bfloat16 [2, 4096, 4096], P(None, 'tensor'), may hold values from -0.09375 to 0.09375
- query_probe: bfloat16 [2, 4096, 4096], P(None, 'dp', 'tensor'), may hold values from -0.09375 to 0.09375
- key_probe: bfloat16 [2, 4096, 1024], P(None, 'dp', 'tensor'), may hold values from -0.09375 to 0.09375
- value_probe: bfloat16 [2, 4096, 1024], P(None, 'dp', 'tensor'), may hold values from -0.09375 to 0.09375
- out_probe: bfloat16 [2, 4096, 4096], P(None, 'tensor', 'dp'), may hold values from -0.09375 to 0.09375
Outputs:
- query_product: float32 [2, 4096, 4096], P(None, 'dp', 'tensor')
- key_product: float32 [2, 4096, 1024], P(None, 'dp', 'tensor')
- value_product: float32 [2, 4096, 1024], P(None, 'dp', 'tensor')
- out_product: float32 [2, 4096, 4096], P(None, 'tensor', 'dp')
The draws below stay inside these ranges and needn't reach their ends.
Inputs may be any that keep to these rules, and one draw needn't show every extreme that they name: lengths[i] counts the leading valid positions of sequence i; the last sequence is full.
All inputs are finite; a program needn't handle non-finite values.
Results may differ from the reference program's by a relative error of at most 0.035.
Values may be sent and summed in bfloat16 or wider, within the bound.
No kernel may reach another device: no remote copies, remote signals or barrier semaphores. Data moves between devices by JAX's collectives and lax.ppermute only.
A program may use at most 128 MiB of HBM per device.

```python
import math
import jax
import jax.numpy as jnp
from jax import lax

D = 4096
HEADS = 32
KVH = 8
HD = 128
LAYERS = 2
LEN = 256
SEQUENCES = 8
TOKENS = 2048
N_DP = 8
N_TENSOR = 16


def draw_tokens(key, part):
    keys = jax.random.split(key, 3)
    row_scale = jnp.exp(jax.random.uniform(keys[1], (TOKENS, 1), jnp.float32, 0.0, math.log(10.0)))
    column_scale = jnp.exp(jax.random.uniform(keys[2], (1, D), jnp.float32, 0.0, math.log(10.0)))
    base = jax.random.truncated_normal(keys[0], -4.0, 4.0, (TOKENS, D), jnp.float32)
    return (0.01 * base * row_scale * column_scale).astype(jnp.bfloat16)


def draw_lengths(key, part):
    number = jnp.arange(SEQUENCES)
    lowest = LEN // 4 + LEN // 2 * number // max(SEQUENCES - 1, 1)
    extra = jax.random.randint(key, (SEQUENCES,), 0, LEN // 4 + 1)
    drawn = jnp.minimum(lowest + extra, LEN)
    return jnp.where(number == SEQUENCES - 1, LEN, drawn).astype(jnp.int32)


def block_scale(stream_key, extent, cuts, smallest, high):
    def one(axis_at, shards_of):
        draws = jax.random.uniform(jax.random.fold_in(jax.random.fold_in(stream_key, 6), axis_at), (shards_of,), jnp.float32, smallest / len(cuts), high / len(cuts))
        return jnp.repeat(jnp.exp(draws), extent[axis_at] // shards_of).reshape((-1,) + (1,) * (len(extent) - axis_at - 1))

    level = one(*cuts[0])
    for cut in cuts[1:]:
        level = level * one(*cut)
    return level


def scatter_about(rng, shape, deviation, reach, cuts=(), kind=jnp.bfloat16):
    gain = block_scale(rng, shape, cuts, -0.22, 0.18) if cuts else 1.0
    values = jax.random.normal(rng, shape, jnp.float32) * deviation * gain
    return jnp.minimum(jnp.maximum(values, -reach), reach).astype(kind)


def setup_inputs(seed: int = 0) -> dict:
    seeds = jax.random.split(jax.random.key(seed), 12)
    tokens = draw_tokens(jax.random.fold_in(seeds[11], 71), 0)
    lengths = draw_lengths(jax.random.fold_in(seeds[11], 71), 0)
    norm_gains = jnp.clip(1.0 + 0.15 * jax.random.normal(seeds[2], (LAYERS, D), jnp.float32), 0.25, 1.75)
    query_weight = scatter_about(seeds[3], (LAYERS, D, HEADS * HD), D ** -0.5, 0.09375, ((2, 16),))
    key_weight = scatter_about(seeds[4], (LAYERS, D, KVH * HD), D ** -0.5, 0.09375, ((2, 16),))
    value_weight = scatter_about(seeds[5], (LAYERS, D, KVH * HD), D ** -0.5, 0.09375, ((2, 16),))
    out_weight = scatter_about(seeds[6], (LAYERS, HEADS * HD, D), (HEADS * HD) ** -0.5, 0.09375, ((1, 16),))
    query_probe = scatter_about(seeds[7], (LAYERS, D, HEADS * HD), D ** -0.5, 0.09375, ((1, 8), (2, 16)))
    key_probe = scatter_about(seeds[8], (LAYERS, D, KVH * HD), D ** -0.5, 0.09375, ((1, 8), (2, 16)))
    value_probe = scatter_about(seeds[9], (LAYERS, D, KVH * HD), D ** -0.5, 0.09375, ((1, 8), (2, 16)))
    out_probe = scatter_about(seeds[10], (LAYERS, HEADS * HD, D), (HEADS * HD) ** -0.5, 0.09375, ((1, 16), (2, 8)))
    return dict(tokens=tokens, lengths=lengths, norm_gains=norm_gains, query_weight=query_weight, key_weight=key_weight, value_weight=value_weight, out_weight=out_weight, query_probe=query_probe, key_probe=key_probe, value_probe=value_probe, out_probe=out_probe)


EPS = 1e-05
THETA = 500000.0

def multiply(pattern, left_side, right_side):
    return jnp.einsum(pattern, left_side.astype(jnp.float32), right_side.astype(jnp.float32))

def matmul(left_side, right_side):
    return jnp.dot(left_side, right_side, preferred_element_type=jnp.float32)

def rope_tables(length, head_size):
    position = jnp.arange(length).astype(jnp.float32)
    column = jnp.arange(head_size // 2).astype(jnp.float32)
    frequency = jnp.exp(-math.log(THETA) * 2.0 * column / head_size)
    angles = position[:, None] * frequency[None, :]
    return (jnp.cos(angles), jnp.sin(angles))

def rotate(values, cosine_table, sine_table, direction):
    middle = values.shape[-1] // 2
    leading = values[..., :middle]
    trailing = values[..., middle:]
    cosine = cosine_table[None, :, None, :]
    sine_part = direction * sine_table[None, :, None, :]
    return jnp.concatenate([leading * cosine - trailing * sine_part, trailing * cosine + leading * sine_part], axis=-1)

def allowed_mask(size, length):
    row_index = jnp.arange(size)[:, None]
    column_index = jnp.arange(size)[None, :]
    return (column_index <= row_index) & (column_index < length)

def attend(queries, key_heads, value_heads, tangent_queries, tangent_keys, tangent_values, length):
    repeat = queries.shape[1] // key_heads.shape[1]
    key_heads = jnp.repeat(key_heads, repeat, axis=1)
    value_heads = jnp.repeat(value_heads, repeat, axis=1)
    tangent_keys = jnp.repeat(tangent_keys, repeat, axis=1)
    tangent_values = jnp.repeat(tangent_values, repeat, axis=1)
    scaling = 1.0 / math.sqrt(queries.shape[-1])
    allowed = allowed_mask(queries.shape[0], length)[None]
    scores = multiply('ihd,jhd->hij', queries, key_heads) * scaling
    powers = jnp.where(allowed, jnp.exp(scores), 0.0)
    weights = powers / lax.optimization_barrier(jnp.sum(powers, axis=-1, keepdims=True))
    weights_low = weights.astype(jnp.bfloat16)
    blended = multiply('hij,jhd->ihd', weights_low, value_heads).astype(jnp.bfloat16)
    tangent_scores = (multiply('ihd,jhd->hij', tangent_queries, key_heads) + multiply('ihd,jhd->hij', queries, tangent_keys)) * scaling
    tangent_weights = weights * (tangent_scores - lax.optimization_barrier(jnp.sum(weights * tangent_scores, axis=-1, keepdims=True)))
    tangent_blended = multiply('hij,jhd->ihd', tangent_weights.astype(jnp.bfloat16), value_heads) + multiply('hij,jhd->ihd', weights_low, tangent_values)
    return (blended, tangent_blended.astype(jnp.bfloat16))

def attend_back(queries, key_heads, value_heads, grad_mixed, length):
    repeat = queries.shape[1] // key_heads.shape[1]
    key_heads = jnp.repeat(key_heads, repeat, axis=1)
    value_heads = jnp.repeat(value_heads, repeat, axis=1)
    scaling = 1.0 / math.sqrt(queries.shape[-1])
    allowed = allowed_mask(queries.shape[0], length)[None]
    scores = multiply('ihd,jhd->hij', queries, key_heads) * scaling
    powers = jnp.where(allowed, jnp.exp(scores), 0.0)
    weights = powers / lax.optimization_barrier(jnp.sum(powers, axis=-1, keepdims=True))
    weights_low = weights.astype(jnp.bfloat16)
    grad_weights = multiply('ihd,jhd->hij', grad_mixed, value_heads)
    grad_values = multiply('hij,ihd->jhd', weights_low, grad_mixed)
    grad_scores = (weights * (grad_weights - lax.optimization_barrier(jnp.sum(weights * grad_weights, axis=-1, keepdims=True))) * scaling).astype(jnp.bfloat16)
    grad_queries = multiply('hij,jhd->ihd', grad_scores, key_heads)
    grad_keys = multiply('hij,ihd->jhd', grad_scores, queries)
    return (grad_queries, grad_keys, grad_values)

def normalize(stream, gain_row):
    wide_stream = stream.astype(jnp.float32)
    inverse = lax.rsqrt(lax.optimization_barrier(jnp.mean(wide_stream * wide_stream, axis=-1, keepdims=True)) + EPS)
    return (wide_stream, inverse, (wide_stream * inverse * gain_row).astype(jnp.bfloat16))

def norm_tangent(wide_stream, inverse, tangent, gain_row):
    shift = lax.optimization_barrier(jnp.mean(wide_stream * tangent, axis=-1, keepdims=True))
    return (gain_row * (tangent * inverse - wide_stream * inverse * inverse * inverse * shift)).astype(jnp.bfloat16)

def norm_back(wide_stream, inverse, grad_normed, gain_row):
    scaled = grad_normed * gain_row
    shift = lax.optimization_barrier(jnp.mean(wide_stream * scaled, axis=-1, keepdims=True))
    return inverse * (scaled - wide_stream * inverse * inverse * shift)

def device_sum(left_terms, right_terms):

    def accumulate(running, pieces):
        partial_value = jnp.zeros_like(running)
        for left_side, right_side in zip(pieces[0], pieces[1]):
            partial_value = partial_value + matmul(left_side, right_side)
        return (running + lax.optimization_barrier(partial_value.astype(jnp.bfloat16)).astype(jnp.float32), None)
    start = jnp.zeros((left_terms[0].shape[1], right_terms[0].shape[2]), jnp.float32)
    running, unused = lax.scan(accumulate, start, (left_terms, right_terms))
    return running

def group_sum(function, arrays, shape):
    batches = tuple((member.reshape((N_DP, member.shape[0] // N_DP) + member.shape[1:]) for member in arrays))

    def accumulate(running, pieces):
        partial_value = function(*pieces)
        return (running + lax.optimization_barrier(partial_value.astype(jnp.bfloat16)).astype(jnp.float32), None)
    running, unused = lax.scan(accumulate, jnp.zeros(shape, jnp.float32), batches)
    return running

def transpose_product(left_side, right_side):
    return matmul(left_side.T, right_side)

def head_pairs(normed_piece, key_piece):
    per_group = multiply('td,tnc->ndc', normed_piece, key_piece)
    group_size = N_TENSOR // KVH
    summed = per_group.reshape(KVH, group_size, per_group.shape[1], per_group.shape[2]).sum(axis=1)
    return summed.transpose(1, 0, 2).reshape(per_group.shape[1], -1)

def reference(tokens, lengths, norm_gains, query_weight, key_weight, value_weight, out_weight, query_probe, key_probe, value_probe, out_probe):
    group_size = N_TENSOR // KVH
    per_device = HEADS // N_TENSOR
    cosine_table, sine_table = rope_tables(LEN, HD)
    token_count = lengths.shape[0] * LEN
    position = jnp.arange(token_count) % LEN
    row_mask = (position < jnp.repeat(lengths, LEN)).astype(jnp.float32)

    def heads_of(values, count):
        return values.reshape(-1, LEN, count, HD)

    def flatten(values):
        return values.reshape(token_count, -1)

    def split_devices(values, columns):
        return values.reshape(token_count, N_TENSOR, columns).transpose(1, 0, 2)
    stream = tokens
    tangent = None
    stored = []
    for layer_index in range(LAYERS):
        gain_row = norm_gains[layer_index].astype(jnp.float32)
        wide_stream, inverse, normed = normalize(stream, gain_row)
        query_primal = matmul(normed, query_weight[layer_index])
        key_primal = matmul(normed, key_weight[layer_index])
        value_primal = matmul(normed, value_weight[layer_index])
        query_moved = matmul(normed, query_probe[layer_index])
        key_moved = matmul(normed, key_probe[layer_index])
        value_moved = matmul(normed, value_probe[layer_index])
        if tangent is not None:
            tangent_normed = norm_tangent(wide_stream, inverse, tangent, gain_row)
            query_moved = query_moved + matmul(tangent_normed, query_weight[layer_index])
            key_moved = key_moved + matmul(tangent_normed, key_weight[layer_index])
            value_moved = value_moved + matmul(tangent_normed, value_weight[layer_index])
        queries = rotate(heads_of(query_primal, HEADS), cosine_table, sine_table, 1.0).astype(jnp.bfloat16)
        key_heads = rotate(heads_of(key_primal, KVH), cosine_table, sine_table, 1.0).astype(jnp.bfloat16)
        value_heads = heads_of(value_primal, KVH).astype(jnp.bfloat16)
        tangent_queries = rotate(heads_of(query_moved, HEADS), cosine_table, sine_table, 1.0).astype(jnp.bfloat16)
        tangent_keys = rotate(heads_of(key_moved, KVH), cosine_table, sine_table, 1.0).astype(jnp.bfloat16)
        tangent_values = heads_of(value_moved, KVH).astype(jnp.bfloat16)
        blended, tangent_blended = lax.map(lambda pieces: attend(*pieces), (queries, key_heads, value_heads, tangent_queries, tangent_keys, tangent_values, lengths))
        blended = flatten(blended)
        tangent_blended = flatten(tangent_blended)
        out_split = out_weight[layer_index].reshape(N_TENSOR, per_device * HD, D)
        probe_split = out_probe[layer_index].reshape(N_TENSOR, per_device * HD, D)
        blended_split = split_devices(blended, per_device * HD)
        tangent_out = device_sum((split_devices(tangent_blended, per_device * HD), blended_split), (out_split, probe_split))
        stored.append((wide_stream, inverse, normed, queries, key_heads, value_heads, blended))
        if layer_index < LAYERS - 1:
            primal_out = device_sum((blended_split,), (out_split,))
            stream = (wide_stream + primal_out).astype(jnp.bfloat16)
        tangent = tangent_out if tangent is None else tangent + tangent_out
    cotangent = row_mask[:, None] * tangent
    query_products = [None] * LAYERS
    key_products = [None] * LAYERS
    value_products = [None] * LAYERS
    out_products = [None] * LAYERS
    for layer_index in reversed(range(LAYERS)):
        wide_stream, inverse, normed, queries, key_heads, value_heads, blended = stored[layer_index]
        cotangent_low = cotangent.astype(jnp.bfloat16)
        out_products[layer_index] = group_sum(transpose_product, (blended, cotangent_low), (HEADS * HD, D))
        grad_mixed = matmul(cotangent_low, out_weight[layer_index].T).astype(jnp.bfloat16)
        grad_queries, grad_keys, grad_values = lax.map(lambda pieces: attend_back(*pieces), (queries, key_heads, value_heads, heads_of(grad_mixed, HEADS), lengths))
        query_low = flatten(rotate(grad_queries, cosine_table, sine_table, -1.0).astype(jnp.bfloat16))
        key_grouped = grad_keys.reshape(-1, LEN, N_TENSOR, per_device, HD).sum(axis=3)
        key_low = rotate(key_grouped, cosine_table, sine_table, -1.0).astype(jnp.bfloat16).reshape(token_count, N_TENSOR, HD)
        value_low = grad_values.reshape(-1, LEN, N_TENSOR, per_device, HD).sum(axis=3).astype(jnp.bfloat16).reshape(token_count, N_TENSOR, HD)
        query_products[layer_index] = group_sum(transpose_product, (normed, query_low), (D, HEADS * HD))
        key_products[layer_index] = group_sum(head_pairs, (normed, key_low), (D, KVH * HD))
        value_products[layer_index] = group_sum(head_pairs, (normed, value_low), (D, KVH * HD))
        if layer_index > 0:
            key_split = jnp.repeat(key_weight[layer_index].reshape(D, KVH, HD).transpose(1, 2, 0), group_size, axis=0)
            value_split = jnp.repeat(value_weight[layer_index].reshape(D, KVH, HD).transpose(1, 2, 0), group_size, axis=0)
            query_split = query_weight[layer_index].T.reshape(N_TENSOR, per_device * HD, D)
            grad_normed = device_sum((split_devices(query_low, per_device * HD), key_low.transpose(1, 0, 2), value_low.transpose(1, 0, 2)), (query_split, key_split, value_split))
            cotangent = cotangent + norm_back(wide_stream, inverse, grad_normed, norm_gains[layer_index].astype(jnp.float32))
    return (jnp.stack(query_products), jnp.stack(key_products), jnp.stack(value_products), jnp.stack(out_products))
```

```python
import functools
import math

import jax
import jax.numpy as jnp
from jax import lax
from jax.experimental import pallas as pl
from jax.experimental.pallas import tpu as pltpu
from jax.sharding import Mesh
from jax.sharding import PartitionSpec as P

HD = 128
LEN = 256
EPS = 1e-05
THETA = 500000.0
DP = ("z", "y")
CHIPS = ("x", "w")
BF = jnp.bfloat16
F32 = jnp.float32


def matmul(left_side, right_side):
    return jnp.dot(left_side, right_side, preferred_element_type=F32)


def contract_rows(left_side, right_side):
    return lax.dot_general(
        left_side, right_side, (((0,), (0,)), ((), ())), preferred_element_type=F32
    )


def contract_last(left_side, right_side):
    return lax.dot_general(
        left_side, right_side, (((1,), (1,)), ((), ())), preferred_element_type=F32
    )


def core_swap(value):
    return lax.ppermute(value, "c", [(0, 1), (1, 0)])


def exchange(pieces, axis):
    return lax.all_to_all(pieces, axis, split_axis=0, concat_axis=0, tiled=True)


def copies(value, axis):
    return jnp.broadcast_to(value[None], (lax.axis_size(axis),) + value.shape)


def gather_rows(share):
    mine = exchange(copies(share, CHIPS), CHIPS).reshape(-1, share.shape[-1])
    return (mine, core_swap(mine))


def sum_rows(own_half, other_half):
    pair = own_half + core_swap(other_half.astype(BF)).astype(F32)
    chips = lax.axis_size(CHIPS)
    pieces = pair.astype(BF).reshape(chips, -1, pair.shape[-1])
    return exchange(pieces, CHIPS).astype(F32).sum(axis=0)


def rope(values, cosine, sine, turn):
    return values * cosine + turn(values) * sine


def half_turn(values):
    return pltpu.roll(values, values.shape[1] // 2, 1)


def attend_kernel(
    size_ref,
    core_ref,
    query_ref,
    own_ref,
    other_ref,
    tangent_query_ref,
    tangent_own_ref,
    tangent_other_ref,
    cosine_ref,
    sine_ref,
    row_ref,
    column_ref,
    blended_ref,
    tangent_ref,
    queries_ref,
    keys_ref,
    values_ref,
    weights_ref,
):
    size = size_ref[0]
    low_core = core_ref[0] == 0
    cosine = cosine_ref[...]
    sine = sine_ref[...]
    lane = lax.broadcasted_iota(jnp.int32, own_ref.shape, 1)
    lower = lane < HD // 2

    def join(own, other):
        first = jnp.where(low_core, own, other)
        second = jnp.where(low_core, other, own)
        key = jnp.where(lower, first, half_turn(second))
        value = jnp.where(lower, half_turn(first), second)
        return rope(key, cosine, sine, half_turn).astype(BF), value.astype(BF)

    key, value = join(own_ref[...], other_ref[...].astype(F32))
    tangent_key, tangent_value = join(tangent_own_ref[...], tangent_other_ref[...].astype(F32))
    keys_ref[...] = key
    values_ref[...] = value
    rows = row_ref[...]
    columns = column_ref[...]
    allowed = (columns <= rows) & (columns < size)
    scaling = 1.0 / math.sqrt(HD)
    for head in range(query_ref.shape[1] // HD):
        at = slice(head * HD, (head + 1) * HD)
        query = rope(query_ref[:, at], cosine, sine, half_turn).astype(BF)
        tangent_query = rope(tangent_query_ref[:, at], cosine, sine, half_turn).astype(BF)
        scores = contract_last(query, key) * scaling
        powers = jnp.where(allowed, jnp.exp(scores), 0.0)
        weights = powers / jnp.sum(powers, axis=-1, keepdims=True)
        weights_low = weights.astype(BF)
        blended_ref[:, at] = matmul(weights_low, value).astype(BF)
        tangent_scores = (
            contract_last(tangent_query, key) + contract_last(query, tangent_key)
        ) * scaling
        shift = jnp.sum(weights * tangent_scores, axis=-1, keepdims=True)
        tangent_weights = (weights * (tangent_scores - shift)).astype(BF)
        tangent_ref[:, at] = (
            matmul(tangent_weights, value) + matmul(weights_low, tangent_value)
        ).astype(BF)
        queries_ref[:, at] = query
        weights_ref[head] = weights


def attend(size, core, query, own, other, tangent_query, tangent_own, tangent_other, tables):
    rows, width = query.shape
    wide = jax.ShapeDtypeStruct((rows, width), BF)
    narrow = jax.ShapeDtypeStruct((rows, HD), BF)
    weights = jax.ShapeDtypeStruct((width // HD, rows, rows), F32)
    smem = pl.BlockSpec(memory_space=pltpu.SMEM)
    vmem = pl.BlockSpec(memory_space=pltpu.VMEM)
    return pl.pallas_call(
        attend_kernel,
        out_shape=(wide, wide, wide, narrow, narrow, weights),
        in_specs=[smem] * 2 + [vmem] * 10,
        out_specs=(vmem,) * 6,
        name="attend",
    )(size, core, query, own, other, tangent_query, tangent_own, tangent_other, *tables)


def attend_back_kernel(
    weights_ref,
    queries_ref,
    keys_ref,
    values_ref,
    grad_ref,
    cosine_ref,
    sine_ref,
    grad_query_ref,
    grad_key_ref,
    grad_value_ref,
):
    cosine = cosine_ref[...]
    sine = -sine_ref[...]
    key = keys_ref[...]
    value = values_ref[...]
    scaling = 1.0 / math.sqrt(HD)
    grad_key = jnp.zeros(key.shape, F32)
    grad_value = jnp.zeros(value.shape, F32)
    for head in range(queries_ref.shape[1] // HD):
        at = slice(head * HD, (head + 1) * HD)
        weights = weights_ref[head]
        grad = grad_ref[:, at]
        grad_weights = contract_last(grad, value)
        grad_value = grad_value + contract_rows(weights.astype(BF), grad)
        shift = jnp.sum(weights * grad_weights, axis=-1, keepdims=True)
        grad_scores = (weights * (grad_weights - shift) * scaling).astype(BF)
        grad_query_ref[:, at] = rope(
            matmul(grad_scores, key), cosine, sine, half_turn
        ).astype(BF)
        grad_key = grad_key + contract_rows(grad_scores, queries_ref[:, at])
    grad_key_ref[...] = rope(grad_key, cosine, sine, half_turn).astype(BF)
    grad_value_ref[...] = grad_value.astype(BF)


def attend_back(weights, queries, keys, values, grad, cosine, sine):
    vmem = pl.BlockSpec(memory_space=pltpu.VMEM)
    return pl.pallas_call(
        attend_back_kernel,
        out_shape=(
            jax.ShapeDtypeStruct(queries.shape, BF),
            jax.ShapeDtypeStruct(keys.shape, BF),
            jax.ShapeDtypeStruct(values.shape, BF),
        ),
        in_specs=[vmem] * 7,
        out_specs=(vmem,) * 3,
        name="attend_back",
    )(weights, queries, keys, values, grad, cosine, sine)


def normalize(stream, gain_row):
    wide_stream = stream.astype(F32)
    inverse = lax.rsqrt(jnp.mean(wide_stream * wide_stream, axis=-1, keepdims=True) + EPS)
    return (wide_stream, inverse, (wide_stream * inverse * gain_row).astype(BF))


def norm_tangent(wide_stream, inverse, tangent, gain_row):
    shift = jnp.mean(wide_stream * tangent, axis=-1, keepdims=True)
    return (
        gain_row * (tangent * inverse - wide_stream * inverse * inverse * inverse * shift)
    ).astype(BF)


def norm_back(wide_stream, inverse, grad_normed, gain_row):
    scaled = grad_normed * gain_row
    shift = jnp.mean(wide_stream * scaled, axis=-1, keepdims=True)
    return inverse * (scaled - wide_stream * inverse * inverse * shift)


def body(
    tokens,
    lengths,
    norm_gains,
    query_weight,
    key_weight,
    value_weight,
    out_weight,
    query_probe,
    key_probe,
    value_probe,
    out_probe,
):
    share_rows, features = tokens.shape
    layer_count, query_width = query_weight.shape[0], query_weight.shape[2]
    half_width = key_weight.shape[2]
    batches = lax.axis_size(DP)
    core = lax.axis_index("c")
    chip = lax.axis_index(CHIPS)
    low_core = core == 0
    rows = LEN
    half = rows // 2
    size = lax.dynamic_slice_in_dim(lengths, lax.axis_index(DP), 1)
    core_word = core.astype(jnp.int32).reshape(1)

    number = jnp.arange(rows)
    owner = jnp.where(number < half, core, 1 - core)
    within = number % half
    position = (within // share_rows) * (2 * share_rows) + owner * share_rows + within % share_rows
    column = jnp.arange(HD // 2).astype(F32)
    frequency = jnp.exp(-math.log(THETA) * 2.0 * column / HD)
    angles = position.astype(F32)[:, None] * frequency[None, :]
    cosine = jnp.concatenate([jnp.cos(angles)] * 2, axis=1)
    sine = jnp.concatenate([-jnp.sin(angles), jnp.sin(angles)], axis=1)
    position = position.astype(jnp.int32)
    tables = (cosine, sine, position[:, None], position[None, :])
    share_position = (chip * 2 + core) * share_rows + jnp.arange(share_rows)
    share_mask = (share_position < size[0]).astype(F32)

    def turned(values):
        return jnp.concatenate([values[half:], values[:half]], axis=0)

    weights = [
        jnp.concatenate([query_weight[n], key_weight[n], value_weight[n]], axis=1)
        for n in range(layer_count)
    ]
    probes = [
        jnp.concatenate([query_probe[n], key_probe[n], value_probe[n]], axis=1)
        for n in range(layer_count)
    ]
    out_turned = [out_probe[n].T for n in range(layer_count)]
    full_probes = [None] * layer_count
    full_out = [None] * layer_count
    full_probes[0] = exchange(copies(probes[0], DP), DP).reshape(features, -1)
    for n in range(layer_count):
        if n > 0:
            full_probes[n] = lax.all_gather(probes[n], DP, axis=0, tiled=True)
        full_out[n] = lax.all_gather(out_turned[n], DP, axis=0, tiled=True)

    stream = tokens
    tangent = None
    stored = []
    all_rows = None
    for n in range(layer_count):
        final_layer = n == layer_count - 1
        gain_row = norm_gains[n]
        wide_stream, inverse, normed = normalize(stream, gain_row)
        if tangent is None:
            normed_halves = gather_rows(normed)
            both = jnp.concatenate(normed_halves, axis=0)
            primal = matmul(both, weights[n])
            moved = matmul(both, full_probes[n])
        else:
            tangent_normed = norm_tangent(wide_stream, inverse, tangent, gain_row)
            joined = gather_rows(jnp.concatenate([normed, tangent_normed], axis=1))
            both = jnp.concatenate([part[:, :features] for part in joined], axis=0)
            tangent_both = jnp.concatenate([part[:, features:] for part in joined], axis=0)
            primal = matmul(both, weights[n])
            moved = matmul(both, full_probes[n]) + matmul(tangent_both, weights[n])
        if n == 0:
            pieces = jnp.moveaxis(both.reshape(rows, batches, -1), 1, 0)
            all_rows = exchange(pieces, DP).reshape(batches * rows, -1)
        own = jnp.concatenate([primal[:, query_width:], moved[:, query_width:]], axis=1)
        other = turned(core_swap(own.astype(BF)))
        blended, tangent_blended, queries, keys, values, attention = attend(
            size,
            core_word,
            primal[:, :query_width],
            own[:, :HD],
            other[:, :HD],
            moved[:, :query_width],
            own[:, HD:],
            other[:, HD:],
            tables,
        )

        def out_terms(at):
            moved_part = matmul(tangent_blended[at], out_weight[n]) + contract_last(
                blended[at], full_out[n]
            )
            if final_layer:
                return moved_part
            return jnp.concatenate([matmul(blended[at], out_weight[n]), moved_part], axis=1)

        other_terms = out_terms(slice(half, rows))
        own_terms = out_terms(slice(0, half))
        sums = sum_rows(own_terms, other_terms)
        stored.append((wide_stream, inverse, both, queries, keys, values, blended, attention))
        if final_layer:
            tangent_sum = sums
        else:
            stream = (wide_stream + sums[:, :features]).astype(BF)
            tangent_sum = sums[:, features:]
        tangent = tangent_sum if tangent is None else tangent + tangent_sum
    cotangent = share_mask[:, None] * tangent
    projected = [None] * layer_count
    out_products = [None] * layer_count
    for n in reversed(range(layer_count)):
        wide_stream, inverse, both, queries, keys, values, blended, attention = stored[n]
        cotangent_both = jnp.concatenate(gather_rows(cotangent.astype(BF)), axis=0)
        grad_mixed = contract_last(cotangent_both, out_weight[n]).astype(BF)
        out_term = contract_rows(cotangent_both, blended).astype(BF)
        out_products[n] = lax.psum_scatter(out_term, DP, scatter_dimension=0, tiled=True)
        query_low, key_low, value_low = attend_back(
            attention, queries, keys, values, grad_mixed, cosine, sine
        )
        key_value = jnp.concatenate([key_low, value_low], axis=1).reshape(rows, 2, 2, half_width)
        own_part = jnp.where(low_core, key_value[:, :, 0], key_value[:, :, 1])
        other_part = jnp.where(low_core, key_value[:, :, 1], key_value[:, :, 0])
        arrived = turned(core_swap(other_part.reshape(rows, -1)))
        pair = (own_part.reshape(rows, -1).astype(F32) + arrived.astype(F32)).astype(BF)
        grads = jnp.concatenate([query_low, pair], axis=1)
        if n > 0:
            own_terms = contract_last(grads[:half], weights[n])
            other_terms = contract_last(grads[half:], weights[n])
            grad_normed = sum_rows(own_terms, other_terms)
            cotangent = cotangent + norm_back(wide_stream, inverse, grad_normed, norm_gains[n])
            term = contract_rows(both, grads).astype(BF)
            projected[n] = lax.psum_scatter(term, DP, scatter_dimension=0, tiled=True).astype(F32)
        else:
            all_grads = exchange(copies(grads, DP), DP).reshape(batches * rows, -1)
            projected[n] = contract_rows(all_rows, all_grads)
    projected = jnp.stack(projected)
    key_end = query_width + half_width
    out_stack = jnp.stack([product.astype(F32).T for product in out_products])
    return (
        projected[:, :, :query_width],
        projected[:, :, query_width:key_end],
        projected[:, :, key_end:],
        out_stack,
    )


def solution(mesh):
    inner = Mesh(mesh.devices.reshape(4, 2, 4, 2, 2), ("z", "y", "x", "w", "c"))
    tensor = ("x", "w", "c")
    placed = (
        P(DP + tensor, None),
        P(),
        P(),
        P(None, None, tensor),
        P(None, None, tensor),
        P(None, None, tensor),
        P(None, tensor, None),
        P(None, DP, tensor),
        P(None, DP, tensor),
        P(None, DP, tensor),
        P(None, tensor, DP),
    )
    return jax.shard_map(
        body,
        mesh=inner,
        in_specs=placed,
        out_specs=(
            P(None, DP, tensor),
            P(None, DP, tensor),
            P(None, DP, tensor),
            P(None, tensor, DP),
        ),
        check_vma=False,
    )
```

```python
import math

import jax
import jax.numpy as jnp
from jax import lax
from jax.experimental import pallas as pl
from jax.experimental.pallas import tpu as pltpu
from jax.sharding import Mesh
from jax.sharding import PartitionSpec as P


HD = 128
LEN = 256
EPS = 1e-05
THETA = 500000.0
DP = ("z", "y")
CHIPS = ("x", "w")
BF = jnp.bfloat16
F32 = jnp.float32


def matmul(left_side, right_side):
    return jnp.dot(left_side, right_side, preferred_element_type=F32)


def contract_rows(left_side, right_side):
    return lax.dot_general(
        left_side, right_side, (((0,), (0,)), ((), ())), preferred_element_type=F32
    )


def contract_last(left_side, right_side):
    return lax.dot_general(
        left_side, right_side, (((1,), (1,)), ((), ())), preferred_element_type=F32
    )


def core_swap(value):
    return lax.ppermute(value, "c", [(0, 1), (1, 0)])


def exchange(pieces, axis):
    return lax.all_to_all(pieces, axis, split_axis=0, concat_axis=0, tiled=True)


def copies(value, axis):
    return jnp.broadcast_to(value[None], (lax.axis_size(axis),) + value.shape)


def beside(own, other, axis):
    first = lax.axis_index(axis) == 0
    return jnp.concatenate(
        [jnp.where(first, own, other), jnp.where(first, other, own)], axis=0
    )


def swap(value, axis):
    return lax.ppermute(value, axis, [(0, 1), (1, 0)])


def ring_blocks(block, axis):
    count = lax.axis_size(axis)
    place = lax.axis_index(axis)
    middle = block.shape[0] // 2
    up = [(source, (source + 1) % count) for source in range(count)]
    down = [(source, (source - 1) % count) for source in range(count)]
    after = lax.ppermute(block, axis, down)
    before = lax.ppermute(block, axis, up)
    far_low = lax.ppermute(after[:middle], axis, down)
    far_high = lax.ppermute(before[middle:], axis, up)
    rows = block.shape[0]
    starts = [((place + step) % count) * rows for step in (0, 1, 3, 2, 2)]
    starts[4] = starts[4] + middle
    return list(zip(starts, (block, after, before, far_low, far_high)))


def block_matmul(left_side, blocks):
    return sum(
        matmul(lax.dynamic_slice_in_dim(left_side, start, block.shape[0], 1), block)
        for start, block in blocks
    )


def own_and_other(both, axis):
    first = lax.axis_index(axis) == 0
    middle = both.shape[0] // 2
    low, high = both[:middle], both[middle:]
    return jnp.where(first, low, high), jnp.where(first, high, low)


def gather_rows(share):
    mine = exchange(copies(share, CHIPS), CHIPS).reshape(-1, share.shape[-1])
    return (mine, core_swap(mine))


def sum_rows(own_half, other_half):
    pair = own_half + core_swap(other_half.astype(BF)).astype(F32)
    chips = lax.axis_size(CHIPS)
    pieces = pair.astype(BF).reshape(chips, -1, pair.shape[-1])
    return exchange(pieces, CHIPS).astype(F32).sum(axis=0)


def rope(values, cosine, sine, turn):
    return values * cosine + turn(values) * sine


def half_turn(values):
    return pltpu.roll(values, values.shape[1] // 2, 1)


def attend_kernel(
    size_ref,
    core_ref,
    primal_ref,
    moved_ref,
    other_ref,
    cosine_ref,
    sine_ref,
    row_ref,
    column_ref,
    blended_ref,
    tangent_ref,
    queries_ref,
    keys_ref,
    values_ref,
    weights_ref,
):
    size = size_ref[0]
    low_core = core_ref[0] == 0
    cosine = cosine_ref[...]
    sine = sine_ref[...]
    count, width = queries_ref.shape
    half = count // 2
    lane = lax.broadcasted_iota(jnp.int32, (count, HD), 1)
    lower = lane < HD // 2

    def join(own, at):
        other = jnp.concatenate([other_ref[half:, at], other_ref[:half, at]], axis=0).astype(F32)
        first = jnp.where(low_core, own, other)
        second = jnp.where(low_core, other, own)
        key = jnp.where(lower, first, half_turn(second))
        value = jnp.where(lower, half_turn(first), second)
        return rope(key, cosine, sine, half_turn).astype(BF), value.astype(BF)

    key, value = join(primal_ref[:, width:], slice(0, HD))
    tangent_key, tangent_value = join(moved_ref[:, width:], slice(HD, 2 * HD))
    keys_ref[...] = key
    values_ref[...] = value
    rows = row_ref[...]
    columns = column_ref[...]
    allowed = (columns <= rows) & (columns < size)
    scaling = 1.0 / math.sqrt(HD)
    for head in range(width // HD):
        at = slice(head * HD, (head + 1) * HD)
        query = rope(primal_ref[:, at], cosine, sine, half_turn).astype(BF)
        tangent_query = rope(moved_ref[:, at], cosine, sine, half_turn).astype(BF)
        scores = contract_last(query, key) * scaling
        powers = jnp.where(allowed, jnp.exp(scores), 0.0)
        weights = powers / jnp.sum(powers, axis=-1, keepdims=True)
        weights_low = weights.astype(BF)
        blended_ref[:, at] = matmul(weights_low, value).astype(BF)
        tangent_scores = (
            contract_last(tangent_query, key) + contract_last(query, tangent_key)
        ) * scaling
        shift = jnp.sum(weights * tangent_scores, axis=-1, keepdims=True)
        tangent_weights = (weights * (tangent_scores - shift)).astype(BF)
        tangent_ref[:, at] = (
            matmul(tangent_weights, value) + matmul(weights_low, tangent_value)
        ).astype(BF)
        queries_ref[:, at] = query
        weights_ref[head] = weights


def attend(size, core, primal, moved, other, tables):
    rows, width = primal.shape
    width = width - HD
    wide = jax.ShapeDtypeStruct((rows, width), BF)
    narrow = jax.ShapeDtypeStruct((rows, HD), BF)
    weights = jax.ShapeDtypeStruct((width // HD, rows, rows), F32)
    smem = pl.BlockSpec(memory_space=pltpu.SMEM)
    vmem = pl.BlockSpec(memory_space=pltpu.VMEM)
    return pl.pallas_call(
        attend_kernel,
        out_shape=(wide, wide, wide, narrow, narrow, weights),
        in_specs=[smem] * 2 + [vmem] * 7,
        out_specs=(vmem,) * 6,
        name="attend",
    )(size, core, primal, moved, other, *tables)


def attend_back_kernel(
    core_ref,
    weights_ref,
    queries_ref,
    keys_ref,
    values_ref,
    grad_ref,
    cosine_ref,
    sine_ref,
    grad_query_ref,
    own_ref,
    other_ref,
):
    low_core = core_ref[0] == 0
    cosine = cosine_ref[...]
    sine = -sine_ref[...]
    key = keys_ref[...]
    value = values_ref[...]
    scaling = 1.0 / math.sqrt(HD)
    grad_key = jnp.zeros(key.shape, F32)
    grad_value = jnp.zeros(value.shape, F32)
    for head in range(queries_ref.shape[1] // HD):
        at = slice(head * HD, (head + 1) * HD)
        weights = weights_ref[head]
        grad = grad_ref[:, at]
        grad_weights = contract_last(grad, value)
        grad_value = grad_value + contract_rows(weights.astype(BF), grad)
        shift = jnp.sum(weights * grad_weights, axis=-1, keepdims=True)
        grad_scores = (weights * (grad_weights - shift) * scaling).astype(BF)
        grad_query_ref[:, at] = rope(
            matmul(grad_scores, key), cosine, sine, half_turn
        ).astype(BF)
        grad_key = grad_key + contract_rows(grad_scores, queries_ref[:, at])
    grad_key = rope(grad_key, cosine, sine, half_turn)
    lower = lax.broadcasted_iota(jnp.int32, grad_key.shape, 1) < HD // 2
    low_part = jnp.where(lower, grad_key, half_turn(grad_value))
    high_part = jnp.where(lower, half_turn(grad_key), grad_value)
    own_ref[...] = jnp.where(low_core, low_part, high_part).astype(BF)
    other_ref[...] = jnp.where(low_core, high_part, low_part).astype(BF)


def attend_back(core, weights, queries, keys, values, grad, cosine, sine):
    smem = pl.BlockSpec(memory_space=pltpu.SMEM)
    vmem = pl.BlockSpec(memory_space=pltpu.VMEM)
    return pl.pallas_call(
        attend_back_kernel,
        out_shape=(
            jax.ShapeDtypeStruct(queries.shape, BF),
            jax.ShapeDtypeStruct(keys.shape, BF),
            jax.ShapeDtypeStruct(values.shape, BF),
        ),
        in_specs=[smem] + [vmem] * 7,
        out_specs=(vmem,) * 3,
        name="attend_back",
    )(core, weights, queries, keys, values, grad, cosine, sine)


def normalize(stream, gain_row):
    wide_stream = stream.astype(F32)
    inverse = lax.rsqrt(jnp.mean(wide_stream * wide_stream, axis=-1, keepdims=True) + EPS)
    return (wide_stream, inverse, (wide_stream * inverse * gain_row).astype(BF))


def norm_tangent(wide_stream, inverse, tangent, gain_row):
    shift = jnp.mean(wide_stream * tangent, axis=-1, keepdims=True)
    return (
        gain_row * (tangent * inverse - wide_stream * inverse * inverse * inverse * shift)
    ).astype(BF)


def norm_back(wide_stream, inverse, grad_normed, gain_row):
    scaled = grad_normed * gain_row
    shift = jnp.mean(wide_stream * scaled, axis=-1, keepdims=True)
    return inverse * (scaled - wide_stream * inverse * inverse * shift)


def program(
    tokens,
    lengths,
    norm_gains,
    query_weight,
    key_weight,
    value_weight,
    out_weight,
    query_probe,
    key_probe,
    value_probe,
    out_probe,
):
    share_rows, features = tokens.shape
    layer_count, query_width = query_weight.shape[0], query_weight.shape[2]
    half_width = key_weight.shape[2]
    batches = lax.axis_size(DP)
    core = lax.axis_index("c")
    chip = lax.axis_index(CHIPS)
    rows = LEN
    half = rows // 2
    size = lax.dynamic_slice_in_dim(lengths, lax.axis_index(DP), 1)
    core_word = core.astype(jnp.int32).reshape(1)

    number = jnp.arange(rows)
    owner = jnp.where(number < half, core, 1 - core)
    within = number % half
    position = (within // share_rows) * (2 * share_rows) + owner * share_rows + within % share_rows
    column = jnp.arange(HD // 2).astype(F32)
    frequency = jnp.exp(-math.log(THETA) * 2.0 * column / HD)
    angles = position.astype(F32)[:, None] * frequency[None, :]
    cosine = jnp.concatenate([jnp.cos(angles)] * 2, axis=1)
    sine = jnp.concatenate([-jnp.sin(angles), jnp.sin(angles)], axis=1)
    position = position.astype(jnp.int32)
    tables = (cosine, sine, position[:, None], position[None, :])
    share_position = (chip * 2 + core) * share_rows + jnp.arange(share_rows)
    share_mask = (share_position < size[0]).astype(F32)

    def turned(values):
        return jnp.concatenate([values[half:], values[:half]], axis=0)

    weights = []
    for n in range(layer_count):
        packed = jnp.concatenate([query_weight[n], key_weight[n], value_weight[n]], axis=1)
        weights.append(lax.optimization_barrier(packed))
    probes = [
        jnp.concatenate([query_probe[n], key_probe[n], value_probe[n]], axis=1)
        for n in range(layer_count)
    ]
    out_turned = [out_probe[n].T for n in range(layer_count)]
    full_probes = [None] * layer_count
    full_out = [None] * layer_count
    arrived = swap(probes[0], "y")
    pair = beside(probes[0], arrived, "y")
    probe_blocks = ring_blocks(pair, "z")
    arrived = swap(out_turned[0], "y")
    pair = beside(out_turned[0], arrived, "y")
    full_out[0] = lax.all_gather(pair, "z", axis=0, tiled=True)
    for n in range(1, layer_count):
        later = jnp.concatenate([probes[n], out_turned[n]], axis=1)
        arrived = swap(later, "y")
        later = beside(later, arrived, "y")
        probe_pair = later[:, : probes[n].shape[1]]
        out_pair = later[:, probes[n].shape[1] :]
        full_probes[n] = lax.all_gather(probe_pair, "z", axis=0, tiled=True)
        full_out[n] = lax.all_gather(out_pair, "z", axis=0, tiled=True)

    stream = tokens
    tangent = None
    stored = []
    all_rows = None
    for n in range(layer_count):
        final_layer = n == layer_count - 1
        gain_row = norm_gains[n]
        wide_stream, inverse, normed = normalize(stream, gain_row)
        if tangent is None:
            normed_halves = gather_rows(normed)
            both = jnp.concatenate(normed_halves, axis=0)
            primal = matmul(both, weights[n])
            moved = block_matmul(both, probe_blocks)
        else:
            tangent_normed = norm_tangent(wide_stream, inverse, tangent, gain_row)
            joined = gather_rows(jnp.concatenate([normed, tangent_normed], axis=0))

            def split(values):
                return values.reshape(-1, 2, share_rows, values.shape[-1])

            both = jnp.concatenate(
                [split(part)[:, 0].reshape(half, features) for part in joined], axis=0
            )
            both = lax.optimization_barrier(both)
            own_way = [split(matmul(part, weights[n])) for part in joined]
            probe_way = [split(matmul(part, full_probes[n])) for part in joined]
            primal = jnp.concatenate(
                [part[:, 0].reshape(half, -1) for part in own_way], axis=0
            )
            moved = jnp.concatenate(
                [
                    (part[:, 1] + probed[:, 0]).reshape(half, -1)
                    for part, probed in zip(own_way, probe_way)
                ],
                axis=0,
            )
        if n == 0:
            pieces = jnp.moveaxis(both.reshape(rows, batches, -1), 1, 0)
            all_rows = exchange(pieces, DP).reshape(batches * rows, -1)
        own = jnp.concatenate([primal[:, query_width:], moved[:, query_width:]], axis=1)
        other = core_swap(own.astype(BF))
        blended, tangent_blended, queries, keys, values, attention = attend(
            size, core_word, primal, moved, other, tables
        )

        def out_terms(at):
            moved_part = matmul(tangent_blended[at], out_weight[n]) + contract_last(
                blended[at], full_out[n]
            )
            if final_layer:
                return moved_part
            return jnp.concatenate([matmul(blended[at], out_weight[n]), moved_part], axis=1)

        other_terms = out_terms(slice(half, rows))
        own_terms = out_terms(slice(0, half))
        sums = sum_rows(own_terms, other_terms)
        stored.append((wide_stream, inverse, both, queries, keys, values, blended, attention))
        if final_layer:
            tangent_sum = sums
        else:
            stream = (wide_stream + sums[:, :features]).astype(BF)
            tangent_sum = sums[:, features:]
        tangent = tangent_sum if tangent is None else tangent + tangent_sum
    cotangent = share_mask[:, None] * tangent
    projected = [None] * layer_count
    out_products = [None] * layer_count
    for n in reversed(range(layer_count)):
        wide_stream, inverse, both, queries, keys, values, blended, attention = stored[n]
        cotangent_both = jnp.concatenate(gather_rows(cotangent.astype(BF)), axis=0)
        grad_mixed = contract_last(cotangent_both, out_weight[n]).astype(BF)
        out_term = contract_rows(cotangent_both, blended).astype(BF)
        partial = lax.psum_scatter(out_term, "z", scatter_dimension=0, tiled=True)
        own_part, other_part = own_and_other(partial, "y")
        arrived = swap(other_part, "y")
        out_products[n] = own_part.astype(F32) + arrived.astype(F32)
        query_low, own_part, other_part = attend_back(
            core_word, attention, queries, keys, values, grad_mixed, cosine, sine
        )
        arrived = turned(core_swap(other_part))
        pair = (own_part.astype(F32) + arrived.astype(F32)).astype(BF)
        grads = jnp.concatenate([query_low, pair], axis=1)
        if n > 0:
            other_terms = contract_last(grads[half:], weights[n])
            own_terms = contract_last(grads[:half], lax.optimization_barrier(weights[n]))
            grad_normed = sum_rows(own_terms, other_terms)
            cotangent = cotangent + norm_back(wide_stream, inverse, grad_normed, norm_gains[n])
            term = contract_rows(both, grads).astype(BF)
            partial = lax.psum_scatter(term, "z", scatter_dimension=0, tiled=True)
            own_part, other_part = own_and_other(partial, "y")
            arrived = swap(other_part, "y")
            projected[n] = own_part.astype(F32) + arrived.astype(F32)
        else:
            arrived = swap(grads, "y")
            blocks = ring_blocks(beside(grads, arrived, "y"), "z")
            projected[n] = sum(
                contract_rows(lax.dynamic_slice_in_dim(all_rows, start, block.shape[0], 0), block)
                for start, block in blocks
            )
    projected = jnp.stack(projected)
    key_end = query_width + half_width
    out_stack = jnp.stack([product.T for product in out_products])
    return (
        projected[:, :, :query_width],
        projected[:, :, query_width:key_end],
        projected[:, :, key_end:],
        out_stack,
    )


def solution(mesh):
    inner = Mesh(mesh.devices.reshape(4, 2, 4, 2, 2), ("z", "y", "x", "w", "c"))
    tensor = ("x", "w", "c")
    placed = (
        P(DP + tensor, None),
        P(),
        P(),
        P(None, None, tensor),
        P(None, None, tensor),
        P(None, None, tensor),
        P(None, tensor, None),
        P(None, DP, tensor),
        P(None, DP, tensor),
        P(None, DP, tensor),
        P(None, tensor, DP),
    )
    return jax.shard_map(
        program,
        mesh=inner,
        in_specs=placed,
        out_specs=(
            P(None, DP, tensor),
            P(None, DP, tensor),
            P(None, DP, tensor),
            P(None, tensor, DP),
        ),
        check_vma=False,
    )
```

```python
import math

import jax
import jax.numpy as jnp
from jax import lax
from jax.experimental import pallas as pl
from jax.experimental.pallas import tpu as pltpu
from jax.sharding import Mesh
from jax.sharding import PartitionSpec as P


HD = 128
LEN = 256
EPS = 1e-05
THETA = 500000.0
DP = ("z", "y")
CHIPS = ("x", "w")
BF = jnp.bfloat16
F32 = jnp.float32


def matmul(left_side, right_side):
    return jnp.dot(left_side, right_side, preferred_element_type=F32)


def contract_rows(left_side, right_side):
    return lax.dot_general(
        left_side, right_side, (((0,), (0,)), ((), ())), preferred_element_type=F32
    )


def contract_last(left_side, right_side):
    return lax.dot_general(
        left_side, right_side, (((1,), (1,)), ((), ())), preferred_element_type=F32
    )


def core_swap(value):
    return lax.ppermute(value, "c", [(0, 1), (1, 0)])


def exchange(pieces, axis):
    return lax.all_to_all(pieces, axis, split_axis=0, concat_axis=0, tiled=True)


def copies(value, axis):
    return jnp.broadcast_to(value[None], (lax.axis_size(axis),) + value.shape)


def beside(own, other, axis):
    first = lax.axis_index(axis) == 0
    return jnp.concatenate(
        [jnp.where(first, own, other), jnp.where(first, other, own)], axis=0
    )


def swap(value, axis):
    return lax.ppermute(value, axis, [(0, 1), (1, 0)])


def ring_blocks(block, axis):
    count = lax.axis_size(axis)
    place = lax.axis_index(axis)
    middle = block.shape[0] // 2
    up = [(source, (source + 1) % count) for source in range(count)]
    down = [(source, (source - 1) % count) for source in range(count)]
    after = lax.ppermute(block, axis, down)
    before = lax.ppermute(block, axis, up)
    far_low = lax.ppermute(after[:middle], axis, down)
    far_high = lax.ppermute(before[middle:], axis, up)
    rows = block.shape[0]
    starts = [((place + step) % count) * rows for step in (0, 1, 3, 2, 2)]
    starts[4] = starts[4] + middle
    return list(zip(starts, (block, after, before, far_low, far_high)))


def block_matmul(left_side, blocks):
    return sum(
        matmul(lax.dynamic_slice_in_dim(left_side, start, block.shape[0], 1), block)
        for start, block in blocks
    )


def own_and_other(both, axis):
    first = lax.axis_index(axis) == 0
    middle = both.shape[0] // 2
    low, high = both[:middle], both[middle:]
    return jnp.where(first, low, high), jnp.where(first, high, low)


def gather_rows(share):
    mine = exchange(copies(share, CHIPS), CHIPS).reshape(-1, share.shape[-1])
    return (mine, core_swap(mine))


def sum_rows(own_half, other_half):
    pair = own_half + core_swap(other_half).astype(F32)
    chips = lax.axis_size(CHIPS)
    pieces = pair.astype(BF).reshape(chips, -1, pair.shape[-1])
    return exchange(pieces, CHIPS).astype(F32).sum(axis=0)


def rope(values, cosine, sine, turn):
    return values * cosine + turn(values) * sine


def half_turn(values):
    return pltpu.roll(values, values.shape[1] // 2, 1)


def join_heads(low_core, own, other_ref, cosine, sine):
    half = own.shape[0] // 2
    other = jnp.concatenate([other_ref[half:], other_ref[:half]], axis=0).astype(F32)
    lower = lax.broadcasted_iota(jnp.int32, own.shape, 1) < HD // 2
    first = jnp.where(low_core, own, other)
    second = jnp.where(low_core, other, own)
    key = jnp.where(lower, first, half_turn(second))
    value = jnp.where(lower, half_turn(first), second)
    return rope(key, cosine, sine, half_turn).astype(BF), value.astype(BF)


def attend_kernel(
    size_ref,
    core_ref,
    primal_ref,
    other_ref,
    cosine_ref,
    sine_ref,
    row_ref,
    column_ref,
    blended_ref,
    queries_ref,
    keys_ref,
    values_ref,
    weights_ref,
):
    size = size_ref[0]
    cosine = cosine_ref[...]
    sine = sine_ref[...]
    width = queries_ref.shape[1]
    key, value = join_heads(core_ref[0] == 0, primal_ref[:, width:], other_ref, cosine, sine)
    keys_ref[...] = key
    values_ref[...] = value
    columns = column_ref[...]
    allowed = (columns <= row_ref[...]) & (columns < size)
    scaling = 1.0 / math.sqrt(HD)
    for head in range(width // HD):
        at = slice(head * HD, (head + 1) * HD)
        query = rope(primal_ref[:, at], cosine, sine, half_turn).astype(BF)
        scores = contract_last(query, key) * scaling
        powers = jnp.where(allowed, jnp.exp(scores), 0.0)
        weights = powers / jnp.sum(powers, axis=-1, keepdims=True)
        blended_ref[:, at] = matmul(weights.astype(BF), value).astype(BF)
        queries_ref[:, at] = query
        weights_ref[head] = weights


def attend(size, core, primal, other, tables):
    rows, width = primal.shape
    width = width - HD
    wide = jax.ShapeDtypeStruct((rows, width), BF)
    narrow = jax.ShapeDtypeStruct((rows, HD), BF)
    weights = jax.ShapeDtypeStruct((width // HD, rows, rows), F32)
    smem = pl.BlockSpec(memory_space=pltpu.SMEM)
    vmem = pl.BlockSpec(memory_space=pltpu.VMEM)
    return pl.pallas_call(
        attend_kernel,
        out_shape=(wide, wide, narrow, narrow, weights),
        in_specs=[smem] * 2 + [vmem] * 6,
        out_specs=(vmem,) * 5,
    )(size, core, primal, other, *tables)


def attend_tangent_kernel(
    core_ref,
    moved_ref,
    other_ref,
    weights_ref,
    queries_ref,
    keys_ref,
    values_ref,
    cosine_ref,
    sine_ref,
    tangent_ref,
):
    cosine = cosine_ref[...]
    sine = sine_ref[...]
    width = queries_ref.shape[1]
    key, value = keys_ref[...], values_ref[...]
    tangent_key, tangent_value = join_heads(
        core_ref[0] == 0, moved_ref[:, width:], other_ref, cosine, sine
    )
    scaling = 1.0 / math.sqrt(HD)
    for head in range(width // HD):
        at = slice(head * HD, (head + 1) * HD)
        tangent_query = rope(moved_ref[:, at], cosine, sine, half_turn).astype(BF)
        weights = weights_ref[head]
        tangent_scores = (
            contract_last(tangent_query, key) + contract_last(queries_ref[:, at], tangent_key)
        ) * scaling
        shift = jnp.sum(weights * tangent_scores, axis=-1, keepdims=True)
        tangent_weights = (weights * (tangent_scores - shift)).astype(BF)
        tangent_ref[:, at] = (
            matmul(tangent_weights, value) + matmul(weights.astype(BF), tangent_value)
        ).astype(BF)


def attend_tangent(core, moved, other, weights, queries, keys, values, cosine, sine):
    smem = pl.BlockSpec(memory_space=pltpu.SMEM)
    vmem = pl.BlockSpec(memory_space=pltpu.VMEM)
    return pl.pallas_call(
        attend_tangent_kernel,
        out_shape=jax.ShapeDtypeStruct(queries.shape, BF),
        in_specs=[smem] + [vmem] * 8,
        out_specs=vmem,
    )(core, moved, other, weights, queries, keys, values, cosine, sine)


def attend_back_kernel(
    core_ref,
    weights_ref,
    queries_ref,
    keys_ref,
    values_ref,
    grad_ref,
    cosine_ref,
    sine_ref,
    grad_query_ref,
    own_ref,
    other_ref,
):
    low_core = core_ref[0] == 0
    cosine = cosine_ref[...]
    sine = -sine_ref[...]
    key = keys_ref[...]
    value = values_ref[...]
    scaling = 1.0 / math.sqrt(HD)
    grad_key = jnp.zeros(key.shape, F32)
    grad_value = jnp.zeros(value.shape, F32)
    for head in range(queries_ref.shape[1] // HD):
        at = slice(head * HD, (head + 1) * HD)
        weights = weights_ref[head]
        grad = grad_ref[:, at]
        grad_weights = contract_last(grad, value)
        grad_value = grad_value + contract_rows(weights.astype(BF), grad)
        shift = jnp.sum(weights * grad_weights, axis=-1, keepdims=True)
        grad_scores = (weights * (grad_weights - shift) * scaling).astype(BF)
        grad_query_ref[:, at] = rope(
            matmul(grad_scores, key), cosine, sine, half_turn
        ).astype(BF)
        grad_key = grad_key + contract_rows(grad_scores, queries_ref[:, at])
    grad_key = rope(grad_key, cosine, sine, half_turn)
    lower = lax.broadcasted_iota(jnp.int32, grad_key.shape, 1) < HD // 2
    low_part = jnp.where(lower, grad_key, half_turn(grad_value))
    high_part = jnp.where(lower, half_turn(grad_key), grad_value)
    own_ref[...] = jnp.where(low_core, low_part, high_part).astype(BF)
    other_ref[...] = jnp.where(low_core, high_part, low_part).astype(BF)


def attend_back(core, weights, queries, keys, values, grad, cosine, sine):
    smem = pl.BlockSpec(memory_space=pltpu.SMEM)
    vmem = pl.BlockSpec(memory_space=pltpu.VMEM)
    return pl.pallas_call(
        attend_back_kernel,
        out_shape=(
            jax.ShapeDtypeStruct(queries.shape, BF),
            jax.ShapeDtypeStruct(keys.shape, BF),
            jax.ShapeDtypeStruct(values.shape, BF),
        ),
        in_specs=[smem] + [vmem] * 7,
        out_specs=(vmem,) * 3,
    )(core, weights, queries, keys, values, grad, cosine, sine)


STEPS = 2


def project_kernel(first_ref, second_ref, query_ref, key_ref, value_ref, out_ref):
    @pl.when(pl.program_id(0) == 0)
    def _():
        out_ref[...] = jnp.zeros_like(out_ref)

    rows = jnp.concatenate([first_ref[...], second_ref[...]], axis=0)
    width = query_ref.shape[2]
    pair = jnp.concatenate([key_ref[0], value_ref[0]], axis=0)
    out_ref[:, :width] += matmul(rows, query_ref[0])
    out_ref[:, width:] += contract_last(rows, pair)


def project(halves, weights, layer):
    query, key, value = weights
    half, features = halves[0].shape
    count = 2 * half
    block = features // STEPS
    width = query.shape[2]
    narrow = key.shape[1]
    return pl.pallas_call(
        project_kernel,
        grid=(STEPS,),
        out_shape=jax.ShapeDtypeStruct((count, width + 2 * narrow), F32),
        in_specs=[
            pl.BlockSpec((half, block), lambda k: (0, k)),
            pl.BlockSpec((half, block), lambda k: (0, k)),
            pl.BlockSpec((1, block, width), lambda k: (layer, k, 0)),
            pl.BlockSpec((1, narrow, block), lambda k: (layer, 0, k)),
            pl.BlockSpec((1, narrow, block), lambda k: (layer, 0, k)),
        ],
        out_specs=pl.BlockSpec((count, width + 2 * narrow), lambda k: (0, 0)),
    )(*halves, query, key, value)


def store_halves(terms, own_ref, other_ref):
    half = terms.shape[0] // 2
    own_ref[...] = terms[:half]
    other_ref[...] = terms[half:].astype(BF)


def project_back_kernel(rows_ref, query_ref, key_ref, value_ref, own_ref, other_ref):
    width = query_ref.shape[2]
    pair = jnp.concatenate([key_ref[0], value_ref[0]], axis=0)
    terms = contract_last(rows_ref[:, :width], query_ref[0]) + matmul(rows_ref[:, width:], pair)
    store_halves(terms, own_ref, other_ref)


def halves_out(count, features):
    block = features // STEPS
    spec = pl.BlockSpec((count // 2, block), lambda k: (0, k))
    return dict(
        grid=(STEPS,),
        out_shape=(
            jax.ShapeDtypeStruct((count // 2, features), F32),
            jax.ShapeDtypeStruct((count // 2, features), BF),
        ),
        out_specs=(spec, spec),
    )


def project_back(rows, weights, layer):
    query, key, value = weights
    count, total = rows.shape
    features, width = query.shape[1:]
    narrow = key.shape[1]
    block = features // STEPS
    return pl.pallas_call(
        project_back_kernel,
        in_specs=[
            pl.BlockSpec((count, total), lambda k: (0, 0)),
            pl.BlockSpec((1, block, width), lambda k: (layer, k, 0)),
            pl.BlockSpec((1, narrow, block), lambda k: (layer, 0, k)),
            pl.BlockSpec((1, narrow, block), lambda k: (layer, 0, k)),
        ],
        **halves_out(count, features),
    )(rows, query, key, value)


def out_kernel(rows_ref, weight_ref, own_ref, other_ref):
    store_halves(matmul(rows_ref[...], weight_ref[0]), own_ref, other_ref)


def out_both_kernel(rows_ref, weight_ref, second_ref, probe_ref, own_ref, other_ref):
    terms = matmul(rows_ref[...], weight_ref[0]) + contract_last(second_ref[...], probe_ref[...])
    store_halves(terms, own_ref, other_ref)


def out_terms(rows, weight, layer, second=None, probe=None):
    count, width = rows.shape
    features = weight.shape[2]
    block = features // STEPS
    whole = pl.BlockSpec((count, width), lambda k: (0, 0))
    specs = [whole, pl.BlockSpec((1, width, block), lambda k: (layer, 0, k))]
    arrays = [rows, weight]
    kernel = out_kernel
    if second is not None:
        specs += [whole, pl.BlockSpec((block, width), lambda k: (k, 0))]
        arrays += [second, probe]
        kernel = out_both_kernel
    return pl.pallas_call(kernel, in_specs=specs, **halves_out(count, features))(*arrays)


def normalize(stream, gain_row):
    wide_stream = stream.astype(F32)
    inverse = lax.rsqrt(jnp.mean(wide_stream * wide_stream, axis=-1, keepdims=True) + EPS)
    return (wide_stream, inverse, (wide_stream * inverse * gain_row).astype(BF))


def norm_tangent(wide_stream, inverse, tangent, gain_row):
    shift = jnp.mean(wide_stream * tangent, axis=-1, keepdims=True)
    return (
        gain_row * (tangent * inverse - wide_stream * inverse * inverse * inverse * shift)
    ).astype(BF)


def norm_back(wide_stream, inverse, grad_normed, gain_row):
    scaled = grad_normed * gain_row
    shift = jnp.mean(wide_stream * scaled, axis=-1, keepdims=True)
    return inverse * (scaled - wide_stream * inverse * inverse * shift)


def program(
    tokens,
    lengths,
    norm_gains,
    query_weight,
    key_weight,
    value_weight,
    out_weight,
    query_probe,
    key_probe,
    value_probe,
    out_probe,
):
    share_rows, _ = tokens.shape
    layer_count, query_width = query_weight.shape[0], query_weight.shape[2]
    half_width = key_weight.shape[2]
    batches = lax.axis_size(DP)
    core = lax.axis_index("c")
    chip = lax.axis_index(CHIPS)
    rows = LEN
    half = rows // 2
    size = lax.dynamic_slice_in_dim(lengths, lax.axis_index(DP), 1)
    core_word = core.astype(jnp.int32).reshape(1)

    number = jnp.arange(rows)
    owner = jnp.where(number < half, core, 1 - core)
    within = number % half
    position = (within // share_rows) * (2 * share_rows) + owner * share_rows + within % share_rows
    column = jnp.arange(HD // 2).astype(F32)
    frequency = jnp.exp(-math.log(THETA) * 2.0 * column / HD)
    angles = position.astype(F32)[:, None] * frequency[None, :]
    cosine = jnp.concatenate([jnp.cos(angles)] * 2, axis=1)
    sine = jnp.concatenate([-jnp.sin(angles), jnp.sin(angles)], axis=1)
    position = position.astype(jnp.int32)
    tables = (cosine, sine, position[:, None], position[None, :])
    share_position = (chip * 2 + core) * share_rows + jnp.arange(share_rows)
    share_mask = (share_position < size[0]).astype(F32)

    def turned(values):
        return jnp.concatenate([values[half:], values[:half]], axis=0)

    weights = (query_weight, key_weight.transpose(0, 2, 1), value_weight.transpose(0, 2, 1))
    probes = [
        jnp.concatenate([query_probe[n], key_probe[n], value_probe[n]], axis=1)
        for n in range(layer_count)
    ]
    out_turned = [out_probe[n].T for n in range(layer_count)]
    full_probes = [None] * layer_count
    full_out = [None] * layer_count
    arrived = swap(probes[0], "y")
    pair = beside(probes[0], arrived, "y")
    probe_blocks = ring_blocks(pair, "z")
    arrived = swap(out_turned[0], "y")
    pair = beside(out_turned[0], arrived, "y")
    full_out[0] = lax.all_gather(pair, "z", axis=0, tiled=True)
    for n in range(1, layer_count):
        later = jnp.concatenate([probes[n], out_turned[n]], axis=1)
        arrived = swap(later, "y")
        later = beside(later, arrived, "y")
        probe_pair = later[:, : probes[n].shape[1]]
        out_pair = later[:, probes[n].shape[1] :]
        full_probes[n] = lax.all_gather(probe_pair, "z", axis=0, tiled=True)
        full_out[n] = lax.all_gather(out_pair, "z", axis=0, tiled=True)

    following = normalize(tokens, norm_gains[0])
    tangent = None
    stored = []
    all_rows = None
    for n in range(layer_count):
        final_layer = n == layer_count - 1
        gain_row = norm_gains[n]
        wide_stream, inverse, normed = following
        normed_halves = gather_rows(normed)
        both = jnp.concatenate(normed_halves, axis=0)
        primal = project(normed_halves, weights, n)
        other = core_swap(primal[:, query_width:].astype(BF))
        blended, queries, keys, values, attention = attend(size, core_word, primal, other, tables)
        if n == 0:
            pieces = jnp.moveaxis(both.reshape(rows, batches, -1), 1, 0)
            all_rows = exchange(pieces, DP).reshape(batches * rows, -1)
        stored.append((wide_stream, inverse, both, queries, keys, values, blended, attention))
        if not final_layer:
            own_terms, other_terms = out_terms(blended, out_weight, n)
            sums = sum_rows(own_terms, other_terms)
            stream = (wide_stream + sums).astype(BF)
            following = normalize(stream, norm_gains[n + 1])
        if tangent is None:
            moved = block_matmul(both, probe_blocks)
        else:
            probed = lax.optimization_barrier(matmul(both, full_probes[n]))
            tangent_normed = norm_tangent(wide_stream, inverse, tangent, gain_row)
            tangent_halves = gather_rows(tangent_normed)
            moved = probed + project(tangent_halves, weights, n)
        other = core_swap(moved[:, query_width:].astype(BF))
        tangent_blended = attend_tangent(
            core_word, moved, other, attention, queries, keys, values, cosine, sine
        )
        own_terms, other_terms = out_terms(tangent_blended, out_weight, n, blended, full_out[n])
        if not final_layer:
            other_terms, _ = lax.optimization_barrier((other_terms, following[2]))
        tangent_sum = sum_rows(own_terms, other_terms)
        tangent = tangent_sum if tangent is None else tangent + tangent_sum
    cotangent = share_mask[:, None] * tangent
    projected = [None] * layer_count
    out_products = [None] * layer_count
    for n in reversed(range(layer_count)):
        wide_stream, inverse, both, queries, keys, values, blended, attention = stored[n]
        cotangent_both = jnp.concatenate(gather_rows(cotangent.astype(BF)), axis=0)
        grad_mixed = contract_last(cotangent_both, out_weight[n]).astype(BF)
        out_term = contract_rows(cotangent_both, blended).astype(BF)
        partial = lax.psum_scatter(out_term, "z", scatter_dimension=0, tiled=True)
        own_part, other_part = own_and_other(partial, "y")
        arrived = swap(other_part, "y")
        out_products[n] = own_part.astype(F32) + arrived.astype(F32)
        query_low, own_part, other_part = attend_back(
            core_word, attention, queries, keys, values, grad_mixed, cosine, sine
        )
        arrived = turned(core_swap(other_part))
        pair = (own_part.astype(F32) + arrived.astype(F32)).astype(BF)
        grads = jnp.concatenate([query_low, pair], axis=1)
        if n > 0:
            own_terms, other_terms = project_back(grads, weights, n)
            grad_normed = sum_rows(own_terms, other_terms)
            cotangent = cotangent + norm_back(wide_stream, inverse, grad_normed, norm_gains[n])
            term = contract_rows(both, grads).astype(BF)
            partial = lax.psum_scatter(term, "z", scatter_dimension=0, tiled=True)
            own_part, other_part = own_and_other(partial, "y")
            arrived = swap(other_part, "y")
            projected[n] = own_part.astype(F32) + arrived.astype(F32)
        else:
            arrived = swap(grads, "y")
            blocks = ring_blocks(beside(grads, arrived, "y"), "z")
            projected[n] = sum(
                contract_rows(lax.dynamic_slice_in_dim(all_rows, start, block.shape[0], 0), block)
                for start, block in blocks
            )
    projected = jnp.stack(projected)
    key_end = query_width + half_width
    out_stack = jnp.stack([product.T for product in out_products])
    return (
        projected[:, :, :query_width],
        projected[:, :, query_width:key_end],
        projected[:, :, key_end:],
        out_stack,
    )


def solution(mesh):
    inner = Mesh(mesh.devices.reshape(4, 2, 4, 2, 2), ("z", "y", "x", "w", "c"))
    tensor = ("x", "w", "c")
    placed = (
        P(DP + tensor, None),
        P(),
        P(),
        P(None, None, tensor),
        P(None, None, tensor),
        P(None, None, tensor),
        P(None, tensor, None),
        P(None, DP, tensor),
        P(None, DP, tensor),
        P(None, DP, tensor),
        P(None, tensor, DP),
    )
    return jax.shard_map(
        program,
        mesh=inner,
        in_specs=placed,
        out_specs=(
            P(None, DP, tensor),
            P(None, DP, tensor),
            P(None, DP, tensor),
            P(None, tensor, DP),
        ),
        check_vma=False,
    )
```

```python
import math

import jax
import jax.numpy as jnp
from jax import lax
from jax.experimental import pallas as pl
from jax.experimental.pallas import tpu as pltpu
from jax.sharding import Mesh
from jax.sharding import PartitionSpec as P


HD = 128
LEN = 256
EPS = 1e-05
THETA = 500000.0
DP = ("z", "y")
CHIPS = ("x", "w")
BF = jnp.bfloat16
F32 = jnp.float32


def matmul(left_side, right_side):
    return jnp.dot(left_side, right_side, preferred_element_type=F32)


def contract_rows(left_side, right_side):
    return lax.dot_general(
        left_side, right_side, (((0,), (0,)), ((), ())), preferred_element_type=F32
    )


def contract_last(left_side, right_side):
    return lax.dot_general(
        left_side, right_side, (((1,), (1,)), ((), ())), preferred_element_type=F32
    )


def core_swap(value):
    return lax.ppermute(value, "c", [(0, 1), (1, 0)])


def exchange(pieces, axis):
    return lax.all_to_all(pieces, axis, split_axis=0, concat_axis=0, tiled=True)


def copies(value, axis):
    return jnp.broadcast_to(value[None], (lax.axis_size(axis),) + value.shape)


def beside(own, other, axis):
    first = lax.axis_index(axis) == 0
    return jnp.concatenate(
        [jnp.where(first, own, other), jnp.where(first, other, own)], axis=0
    )


def swap(value, axis):
    return lax.ppermute(value, axis, [(0, 1), (1, 0)])


def ring_blocks(block, axis):
    count = lax.axis_size(axis)
    place = lax.axis_index(axis)
    middle = block.shape[0] // 2
    up = [(source, (source + 1) % count) for source in range(count)]
    down = [(source, (source - 1) % count) for source in range(count)]
    after = lax.ppermute(block, axis, down)
    before = lax.ppermute(block, axis, up)
    far_low = lax.ppermute(after[:middle], axis, down)
    far_high = lax.ppermute(before[middle:], axis, up)
    rows = block.shape[0]
    starts = [((place + step) % count) * rows for step in (0, 1, 3, 2, 2)]
    starts[4] = starts[4] + middle
    return list(zip(starts, (block, after, before, far_low, far_high)))


def block_matmul(left_side, blocks):
    return sum(
        matmul(lax.dynamic_slice_in_dim(left_side, start, block.shape[0], 1), block)
        for start, block in blocks
    )


def own_and_other(both, axis):
    first = lax.axis_index(axis) == 0
    middle = both.shape[0] // 2
    low, high = both[:middle], both[middle:]
    return jnp.where(first, low, high), jnp.where(first, high, low)


def gather_rows(share):
    mine = exchange(copies(share, CHIPS), CHIPS).reshape(-1, share.shape[-1])
    return (mine, core_swap(mine))


def sum_rows(own_half, other_half):
    pair = own_half.astype(F32) + core_swap(other_half).astype(F32)
    chips = lax.axis_size(CHIPS)
    pieces = pair.astype(BF).reshape(chips, -1, pair.shape[-1])
    return exchange(pieces, CHIPS).astype(F32).sum(axis=0)


def rope(values, cosine, sine, turn):
    return values * cosine + turn(values) * sine


def half_turn(values):
    return pltpu.roll(values, values.shape[1] // 2, 1)


def join_heads(low_core, own, other_ref, cosine, sine):
    half = own.shape[0] // 2
    other = jnp.concatenate([other_ref[half:], other_ref[:half]], axis=0).astype(F32)
    lower = lax.broadcasted_iota(jnp.int32, own.shape, 1) < HD // 2
    first = jnp.where(low_core, own, other)
    second = jnp.where(low_core, other, own)
    key = jnp.where(lower, first, half_turn(second))
    value = jnp.where(lower, half_turn(first), second)
    return rope(key, cosine, sine, half_turn).astype(BF), value.astype(BF)


def attend_kernel(
    size_ref,
    core_ref,
    primal_ref,
    other_ref,
    cosine_ref,
    sine_ref,
    row_ref,
    column_ref,
    blended_ref,
    queries_ref,
    keys_ref,
    values_ref,
    weights_ref,
):
    size = size_ref[0]
    cosine = cosine_ref[...]
    sine = sine_ref[...]
    width = queries_ref.shape[1]
    key, value = join_heads(core_ref[0] == 0, primal_ref[:, width:], other_ref, cosine, sine)
    keys_ref[...] = key
    values_ref[...] = value
    columns = column_ref[...]
    allowed = (columns <= row_ref[...]) & (columns < size)
    scaling = 1.0 / math.sqrt(HD)
    for head in range(width // HD):
        at = slice(head * HD, (head + 1) * HD)
        query = rope(primal_ref[:, at], cosine, sine, half_turn).astype(BF)
        scores = contract_last(query, key) * scaling
        powers = jnp.where(allowed, jnp.exp(scores), 0.0)
        weights = powers / jnp.sum(powers, axis=-1, keepdims=True)
        blended_ref[:, at] = matmul(weights.astype(BF), value).astype(BF)
        queries_ref[:, at] = query
        weights_ref[head] = weights


def attend(size, core, primal, other, tables):
    rows, width = primal.shape
    width = width - HD
    wide = jax.ShapeDtypeStruct((rows, width), BF)
    narrow = jax.ShapeDtypeStruct((rows, HD), BF)
    weights = jax.ShapeDtypeStruct((width // HD, rows, rows), F32)
    smem = pl.BlockSpec(memory_space=pltpu.SMEM)
    vmem = pl.BlockSpec(memory_space=pltpu.VMEM)
    return pl.pallas_call(
        attend_kernel,
        out_shape=(wide, wide, narrow, narrow, weights),
        in_specs=[smem] * 2 + [vmem] * 6,
        out_specs=(vmem,) * 5,
    )(size, core, primal, other, *tables)


def attend_tangent_kernel(
    core_ref,
    moved_ref,
    other_ref,
    weights_ref,
    queries_ref,
    keys_ref,
    values_ref,
    cosine_ref,
    sine_ref,
    tangent_ref,
):
    cosine = cosine_ref[...]
    sine = sine_ref[...]
    width = queries_ref.shape[1]
    key, value = keys_ref[...], values_ref[...]
    tangent_key, tangent_value = join_heads(
        core_ref[0] == 0, moved_ref[:, width:], other_ref, cosine, sine
    )
    scaling = 1.0 / math.sqrt(HD)
    for head in range(width // HD):
        at = slice(head * HD, (head + 1) * HD)
        tangent_query = rope(moved_ref[:, at], cosine, sine, half_turn).astype(BF)
        weights = weights_ref[head]
        tangent_scores = (
            contract_last(tangent_query, key) + contract_last(queries_ref[:, at], tangent_key)
        ) * scaling
        shift = jnp.sum(weights * tangent_scores, axis=-1, keepdims=True)
        tangent_weights = (weights * (tangent_scores - shift)).astype(BF)
        tangent_ref[:, at] = (
            matmul(tangent_weights, value) + matmul(weights.astype(BF), tangent_value)
        ).astype(BF)


def attend_tangent(core, moved, other, weights, queries, keys, values, cosine, sine):
    smem = pl.BlockSpec(memory_space=pltpu.SMEM)
    vmem = pl.BlockSpec(memory_space=pltpu.VMEM)
    return pl.pallas_call(
        attend_tangent_kernel,
        out_shape=jax.ShapeDtypeStruct(queries.shape, BF),
        in_specs=[smem] + [vmem] * 8,
        out_specs=vmem,
    )(core, moved, other, weights, queries, keys, values, cosine, sine)


def attend_back_kernel(
    core_ref,
    weights_ref,
    queries_ref,
    keys_ref,
    values_ref,
    grad_ref,
    cosine_ref,
    sine_ref,
    grad_query_ref,
    own_ref,
    other_ref,
):
    low_core = core_ref[0] == 0
    cosine = cosine_ref[...]
    sine = -sine_ref[...]
    key = keys_ref[...]
    value = values_ref[...]
    scaling = 1.0 / math.sqrt(HD)
    grad_key = jnp.zeros(key.shape, F32)
    grad_value = jnp.zeros(value.shape, F32)
    for head in range(queries_ref.shape[1] // HD):
        at = slice(head * HD, (head + 1) * HD)
        weights = weights_ref[head]
        grad = grad_ref[:, at]
        grad_weights = contract_last(grad, value)
        grad_value = grad_value + contract_rows(weights.astype(BF), grad)
        shift = jnp.sum(weights * grad_weights, axis=-1, keepdims=True)
        grad_scores = (weights * (grad_weights - shift) * scaling).astype(BF)
        grad_query_ref[:, at] = rope(
            matmul(grad_scores, key), cosine, sine, half_turn
        ).astype(BF)
        grad_key = grad_key + contract_rows(grad_scores, queries_ref[:, at])
    grad_key = rope(grad_key, cosine, sine, half_turn)
    lower = lax.broadcasted_iota(jnp.int32, grad_key.shape, 1) < HD // 2
    low_part = jnp.where(lower, grad_key, half_turn(grad_value))
    high_part = jnp.where(lower, half_turn(grad_key), grad_value)
    own_ref[...] = jnp.where(low_core, low_part, high_part).astype(BF)
    other_ref[...] = jnp.where(low_core, high_part, low_part).astype(BF)


def attend_back(core, weights, queries, keys, values, grad, cosine, sine):
    smem = pl.BlockSpec(memory_space=pltpu.SMEM)
    vmem = pl.BlockSpec(memory_space=pltpu.VMEM)
    return pl.pallas_call(
        attend_back_kernel,
        out_shape=(
            jax.ShapeDtypeStruct(queries.shape, BF),
            jax.ShapeDtypeStruct(keys.shape, BF),
            jax.ShapeDtypeStruct(values.shape, BF),
        ),
        in_specs=[smem] + [vmem] * 7,
        out_specs=(vmem,) * 3,
    )(core, weights, queries, keys, values, grad, cosine, sine)


STEPS = 2


def project_kernel(first_ref, second_ref, query_ref, key_ref, value_ref, out_ref):
    @pl.when(pl.program_id(0) == 0)
    def _():
        out_ref[...] = jnp.zeros_like(out_ref)

    rows = jnp.concatenate([first_ref[...], second_ref[...]], axis=0)
    width = query_ref.shape[2]
    pair = jnp.concatenate([key_ref[0], value_ref[0]], axis=0)
    out_ref[:, :width] += matmul(rows, query_ref[0])
    out_ref[:, width:] += contract_last(rows, pair)


def project(halves, weights, layer):
    query, key, value = weights
    half, features = halves[0].shape
    count = 2 * half
    block = features // STEPS
    width = query.shape[2]
    narrow = key.shape[1]
    return pl.pallas_call(
        project_kernel,
        grid=(STEPS,),
        out_shape=jax.ShapeDtypeStruct((count, width + 2 * narrow), F32),
        in_specs=[
            pl.BlockSpec((half, block), lambda k: (0, k)),
            pl.BlockSpec((half, block), lambda k: (0, k)),
            pl.BlockSpec((1, block, width), lambda k: (layer, k, 0)),
            pl.BlockSpec((1, narrow, block), lambda k: (layer, 0, k)),
            pl.BlockSpec((1, narrow, block), lambda k: (layer, 0, k)),
        ],
        out_specs=pl.BlockSpec((count, width + 2 * narrow), lambda k: (0, 0)),
    )(*halves, query, key, value)


def store_halves(terms, own_ref, other_ref):
    half = terms.shape[0] // 2
    own_ref[...] = terms[:half].astype(BF)
    other_ref[...] = terms[half:].astype(BF)


def project_back_kernel(rows_ref, query_ref, key_ref, value_ref, own_ref, other_ref):
    width = query_ref.shape[2]
    pair = jnp.concatenate([key_ref[0], value_ref[0]], axis=0)
    terms = contract_last(rows_ref[:, :width], query_ref[0]) + matmul(rows_ref[:, width:], pair)
    store_halves(terms, own_ref, other_ref)


def halves_out(count, features):
    block = features // STEPS
    spec = pl.BlockSpec((count // 2, block), lambda k: (0, k))
    return dict(
        grid=(STEPS,),
        out_shape=(
            jax.ShapeDtypeStruct((count // 2, features), BF),
            jax.ShapeDtypeStruct((count // 2, features), BF),
        ),
        out_specs=(spec, spec),
    )


def project_back(rows, weights, layer):
    query, key, value = weights
    count, total = rows.shape
    features, width = query.shape[1:]
    narrow = key.shape[1]
    block = features // STEPS
    return pl.pallas_call(
        project_back_kernel,
        in_specs=[
            pl.BlockSpec((count, total), lambda k: (0, 0)),
            pl.BlockSpec((1, block, width), lambda k: (layer, k, 0)),
            pl.BlockSpec((1, narrow, block), lambda k: (layer, 0, k)),
            pl.BlockSpec((1, narrow, block), lambda k: (layer, 0, k)),
        ],
        **halves_out(count, features),
    )(rows, query, key, value)


def out_kernel(rows_ref, weight_ref, own_ref, other_ref):
    store_halves(matmul(rows_ref[...], weight_ref[0]), own_ref, other_ref)


def out_both_kernel(rows_ref, weight_ref, second_ref, probe_ref, own_ref, other_ref):
    terms = matmul(rows_ref[...], weight_ref[0]) + contract_last(second_ref[...], probe_ref[...])
    store_halves(terms, own_ref, other_ref)


def out_terms(rows, weight, layer, second=None, probe=None):
    count, width = rows.shape
    features = weight.shape[2]
    block = features // STEPS
    whole = pl.BlockSpec((count, width), lambda k: (0, 0))
    specs = [whole, pl.BlockSpec((1, width, block), lambda k: (layer, 0, k))]
    arrays = [rows, weight]
    kernel = out_kernel
    if second is not None:
        specs += [whole, pl.BlockSpec((block, width), lambda k: (k, 0))]
        arrays += [second, probe]
        kernel = out_both_kernel
    return pl.pallas_call(kernel, in_specs=specs, **halves_out(count, features))(*arrays)


def normalize(stream, gain_row):
    wide_stream = stream.astype(F32)
    inverse = lax.rsqrt(jnp.mean(wide_stream * wide_stream, axis=-1, keepdims=True) + EPS)
    return (wide_stream, inverse, (wide_stream * inverse * gain_row).astype(BF))


def norm_tangent(wide_stream, inverse, tangent, gain_row):
    shift = jnp.mean(wide_stream * tangent, axis=-1, keepdims=True)
    return (
        gain_row * (tangent * inverse - wide_stream * inverse * inverse * inverse * shift)
    ).astype(BF)


def norm_back(wide_stream, inverse, grad_normed, gain_row):
    scaled = grad_normed * gain_row
    shift = jnp.mean(wide_stream * scaled, axis=-1, keepdims=True)
    return inverse * (scaled - wide_stream * inverse * inverse * shift)


def program(
    tokens,
    lengths,
    norm_gains,
    query_weight,
    key_weight,
    value_weight,
    out_weight,
    query_probe,
    key_probe,
    value_probe,
    out_probe,
):
    share_rows, _ = tokens.shape
    layer_count, query_width = query_weight.shape[0], query_weight.shape[2]
    half_width = key_weight.shape[2]
    batches = lax.axis_size(DP)
    core = lax.axis_index("c")
    chip = lax.axis_index(CHIPS)
    rows = LEN
    half = rows // 2
    size = lax.dynamic_slice_in_dim(lengths, lax.axis_index(DP), 1)
    core_word = core.astype(jnp.int32).reshape(1)

    number = jnp.arange(rows)
    owner = jnp.where(number < half, core, 1 - core)
    within = number % half
    position = (within // share_rows) * (2 * share_rows) + owner * share_rows + within % share_rows
    column = jnp.arange(HD // 2).astype(F32)
    frequency = jnp.exp(-math.log(THETA) * 2.0 * column / HD)
    angles = position.astype(F32)[:, None] * frequency[None, :]
    cosine = jnp.concatenate([jnp.cos(angles)] * 2, axis=1)
    sine = jnp.concatenate([-jnp.sin(angles), jnp.sin(angles)], axis=1)
    position = position.astype(jnp.int32)
    tables = (cosine, sine, position[:, None], position[None, :])
    share_position = (chip * 2 + core) * share_rows + jnp.arange(share_rows)
    share_mask = (share_position < size[0]).astype(F32)

    def turned(values):
        return jnp.concatenate([values[half:], values[:half]], axis=0)

    weights = (query_weight, key_weight.transpose(0, 2, 1), value_weight.transpose(0, 2, 1))
    probes = [
        jnp.concatenate([query_probe[n], key_probe[n], value_probe[n]], axis=1)
        for n in range(layer_count)
    ]
    out_turned = [out_probe[n].T for n in range(layer_count)]
    full_probes = [None] * layer_count
    full_out = [None] * layer_count
    arrived = swap(probes[0], "y")
    pair = beside(probes[0], arrived, "y")
    probe_blocks = ring_blocks(pair, "z")
    arrived = swap(out_turned[0], "y")
    pair = beside(out_turned[0], arrived, "y")
    full_out[0] = lax.all_gather(pair, "z", axis=0, tiled=True)
    for n in range(1, layer_count):
        later = jnp.concatenate([probes[n], out_turned[n]], axis=1)
        arrived = swap(later, "y")
        later = beside(later, arrived, "y")
        probe_pair = later[:, : probes[n].shape[1]]
        out_pair = later[:, probes[n].shape[1] :]
        full_probes[n] = lax.all_gather(probe_pair, "z", axis=0, tiled=True)
        full_out[n] = lax.all_gather(out_pair, "z", axis=0, tiled=True)

    following = normalize(tokens, norm_gains[0])
    tangent = None
    stored = []
    all_rows = None
    for n in range(layer_count):
        final_layer = n == layer_count - 1
        gain_row = norm_gains[n]
        wide_stream, inverse, normed = following
        normed_halves = gather_rows(normed)
        both = jnp.concatenate(normed_halves, axis=0)
        primal = project(normed_halves, weights, n)
        other = core_swap(primal[:, query_width:].astype(BF))
        blended, queries, keys, values, attention = attend(size, core_word, primal, other, tables)
        if n == 0:
            pieces = jnp.moveaxis(both.reshape(rows, batches, -1), 1, 0)
            all_rows = exchange(pieces, DP).reshape(batches * rows, -1)
        stored.append((wide_stream, inverse, both, queries, keys, values, blended, attention))
        if not final_layer:
            own_terms, other_terms = out_terms(blended, out_weight, n)
            sums = sum_rows(own_terms, other_terms)
            stream = (wide_stream + sums).astype(BF)
            following = normalize(stream, norm_gains[n + 1])
        if tangent is None:
            moved = block_matmul(both, probe_blocks)
        else:
            probed = lax.optimization_barrier(matmul(both, full_probes[n]))
            tangent_normed = norm_tangent(wide_stream, inverse, tangent, gain_row)
            tangent_halves = gather_rows(tangent_normed)
            moved = probed + project(tangent_halves, weights, n)
        other = core_swap(moved[:, query_width:].astype(BF))
        tangent_blended = attend_tangent(
            core_word, moved, other, attention, queries, keys, values, cosine, sine
        )
        own_terms, other_terms = out_terms(tangent_blended, out_weight, n, blended, full_out[n])
        if not final_layer:
            other_terms, _ = lax.optimization_barrier((other_terms, following[2]))
        tangent_sum = sum_rows(own_terms, other_terms)
        tangent = tangent_sum if tangent is None else tangent + tangent_sum
    cotangent = share_mask[:, None] * tangent
    projected = [None] * layer_count
    out_products = [None] * layer_count
    for n in reversed(range(layer_count)):
        wide_stream, inverse, both, queries, keys, values, blended, attention = stored[n]
        cotangent_both = jnp.concatenate(gather_rows(cotangent.astype(BF)), axis=0)
        grad_mixed = contract_last(cotangent_both, out_weight[n]).astype(BF)
        out_term = contract_rows(cotangent_both, blended).astype(BF)
        partial = lax.psum_scatter(out_term, "z", scatter_dimension=0, tiled=True)
        own_part, other_part = own_and_other(partial, "y")
        arrived = swap(other_part, "y")
        out_products[n] = own_part.astype(F32) + arrived.astype(F32)
        query_low, own_part, other_part = attend_back(
            core_word, attention, queries, keys, values, grad_mixed, cosine, sine
        )
        arrived = turned(core_swap(other_part))
        pair = (own_part.astype(F32) + arrived.astype(F32)).astype(BF)
        grads = jnp.concatenate([query_low, pair], axis=1)
        if n > 0:
            own_terms, other_terms = project_back(grads, weights, n)
            grad_normed = sum_rows(own_terms, other_terms)
            cotangent = cotangent + norm_back(wide_stream, inverse, grad_normed, norm_gains[n])
            term = contract_rows(both, grads).astype(BF)
            partial = lax.psum_scatter(term, "z", scatter_dimension=0, tiled=True)
            own_part, other_part = own_and_other(partial, "y")
            arrived = swap(other_part, "y")
            projected[n] = own_part.astype(F32) + arrived.astype(F32)
        else:
            arrived = swap(grads, "y")
            blocks = ring_blocks(beside(grads, arrived, "y"), "z")
            projected[n] = sum(
                contract_rows(lax.dynamic_slice_in_dim(all_rows, start, block.shape[0], 0), block)
                for start, block in blocks
            )
    projected = jnp.stack(projected)
    key_end = query_width + half_width
    out_stack = jnp.stack([product.T for product in out_products])
    return (
        projected[:, :, :query_width],
        projected[:, :, query_width:key_end],
        projected[:, :, key_end:],
        out_stack,
    )


def solution(mesh):
    inner = Mesh(mesh.devices.reshape(4, 2, 4, 2, 2), ("z", "y", "x", "w", "c"))
    tensor = ("x", "w", "c")
    placed = (
        P(DP + tensor, None),
        P(),
        P(),
        P(None, None, tensor),
        P(None, None, tensor),
        P(None, None, tensor),
        P(None, tensor, None),
        P(None, DP, tensor),
        P(None, DP, tensor),
        P(None, DP, tensor),
        P(None, tensor, DP),
    )
    return jax.shard_map(
        program,
        mesh=inner,
        in_specs=placed,
        out_specs=(
            P(None, DP, tensor),
            P(None, DP, tensor),
            P(None, DP, tensor),
            P(None, tensor, DP),
        ),
        check_vma=False,
    )
```
